32 devices in a mesh: dp: 2 (over x), expert: 4 (over z), tensor: 4 (over y, core).
Axes of the slice: x: 2, y: 2, z: 4, core: 2. Of those that a mesh axis runs over, the one named last changes fastest.
Arguments:
- tokens: bfloat16 [256, 3072], P(('dp', 'expert', 'tensor')), parts along dimension 0, may hold values from -6 to 6
- expert_ids: int32 [256, 2], P(('dp', 'expert', 'tensor')), parts along dimension 0, may hold values from 0 to 3, all different within a row; in each aligned block of 8 rows (0 to 7, 8 to 15, ...) at most 8 rows name the same one
- gate_weights: float32 [256, 2], P(('dp', 'expert', 'tensor')), parts along dimension 0, may hold values from 0.2 to 1
- gate_proj: bfloat16 [4, 3072, 8192], P('expert', None, 'tensor'), may hold values from -0.109375 to 0.109375
- up_proj: bfloat16 [4, 3072, 8192], P('expert', None, 'tensor'), may hold values from -0.109375 to 0.109375
- down_proj: bfloat16 [4, 8192, 3072], P('expert', 'tensor'), may hold values from -0.0625 to 0.0625
Outputs:
- mixture: bfloat16 [256, 3072], P(('dp', 'expert', 'tensor')), parts along dimension 0
The draws below stay inside these ranges and needn't reach their ends.
There are 2 independent parts, one for each index of `dp`. The reference program is written for one: setup_inputs(seed, part) draws one part's arguments, and reference() takes and returns one part's arrays. A program takes and returns all parts, laid end to end along the dimension named above; an argument that names none is the same for every part. Nothing has to cross between parts.
Inputs may be any that keep to these rules, and one draw needn't show every extreme that they name: `expert_ids`: each token names two different experts; no expert is named by more than 8 tokens of one device (aligned blocks of 8 rows), and some blocks reach this bound.
All inputs are finite; a program needn't handle non-finite values.
Results may differ from the reference program's by a relative error of at most 0.015.
Values may be sent and summed in bfloat16 or wider, within the bound.
A program may use at most 64 MiB of HBM per device.

```python
import math
import jax
import jax.numpy as jnp
import numpy as np
from jax import lax

D = 3072
FF = 8192
TOK_DEV = 8
EXPERTS = 4
TOKENS = 128
CAP = 8
N_TENSOR = 4


def levels(key, extent, cuts, low, top_value):
    def one(dim, shards_of):
        draws = jax.random.uniform(jax.random.fold_in(jax.random.fold_in(key, 6), dim), (shards_of,), jnp.float32, low / len(cuts), top_value / len(cuts))
        return jnp.repeat(jnp.exp(draws), extent[dim] // shards_of).reshape((-1,) + (1,) * (len(extent) - dim - 1))

    level = one(*cuts[0])
    for cut in cuts[1:]:
        level = level * one(*cut)
    return level


def assign_block(key, own, number, rows, count, top, most, skew):
    order = jax.random.permutation(key, count)
    packed, usual = shares(count, rows * top, most, skew, True), shares(count, rows * top, most, skew, False)
    places = jnp.arange(count)

    def named(lengths, rotation):
        used = int((lengths > 0).sum())
        fixed = max(1, used // 4)
        moved = fixed + (places - fixed + rotation * (used - fixed)) % max(1, count - fixed)
        return jnp.zeros((count,), jnp.int32).at[order[jnp.where(places < fixed, places, moved)]].set(jnp.asarray(lengths, jnp.int32))

    lengths = jnp.where(number % 4 == 0, named(packed, number // 4), named(usual, number - number // 4 - 1))
    mixed = jax.random.permutation(jax.random.fold_in(own, 3), count)
    donor, taker = mixed[0:count // 2 * 2:2], mixed[1:count // 2 * 2:2]
    margin = jnp.minimum(lengths[donor] - 1, most - lengths[taker]) // 2
    margin = jnp.where((donor == order[0]) | (taker == order[0]) | (lengths[taker] == 0), 0, jnp.maximum(margin, 0))
    moved = jax.random.randint(jax.random.fold_in(own, 4), (count // 2,), 0, 1 << 20) % (margin + 1)
    lengths = lengths.at[donor].add(-moved).at[taker].add(moved)
    items = jnp.searchsorted(jnp.cumsum(lengths), jnp.arange(rows * top), side="right").astype(jnp.int32)
    grid = items.reshape(top, rows).T
    grid = grid[jax.random.permutation(jax.random.fold_in(own, 1), rows)]
    rotation = jax.random.randint(jax.random.fold_in(own, 2), (rows, 1), 0, top)
    return jnp.take_along_axis(grid, (jnp.arange(top)[None, :] + rotation) % top, axis=1)


def shares(count, total, limit, lean, full):
    portions = [(1 << 20) // math.isqrt(rank ** lean) + 1 for rank in range(1, count + 1)]
    largest = limit if full else min(limit, max(-(-total // count), total * portions[0] // sum(portions)))
    least = 1 if total - largest >= count - 1 else 0
    holding, spare = [largest] + [least] * (count - 1), total - largest - least * (count - 1)
    while spare > 0:
        candidates = [i for i in range(1, count) if holding[i] < largest] or [i for i in range(1, count) if holding[i] < limit]
        whole, budget = sum([portions[i] for i in candidates]), spare
        for i in candidates:
            more = min(limit - holding[i], max(1, budget * portions[i] // whole), spare)
            holding[i] = holding[i] + more
            spare = spare - more
    return np.array(holding)


def scatter_about(stream_key, extent, scale, limit, pieces=(), kind=jnp.bfloat16):
    result = jax.random.normal(stream_key, extent, jnp.float32) * scale
    if len(pieces) > 0:
        result = levels(stream_key, extent, pieces, -0.22, 0.18) * result
    return jnp.clip(result, min=-limit, max=limit).astype(kind)


def setup_inputs(seed: int = 0, part: int = 0) -> dict:
    arg_keys = jax.random.split(jax.random.key(seed), 7)
    own_keys = jax.random.split(jax.random.fold_in(arg_keys[6], part), 7)
    tokens = scatter_about(own_keys[0], (TOKENS, D), 1.0, 6.0, ((0, 16),))
    expert_ids_keys = jax.random.split(jax.random.fold_in(own_keys[1], 1), TOKENS // TOK_DEV)
    expert_ids_turns = jax.random.permutation(jax.random.fold_in(own_keys[1], 3), TOKENS // TOK_DEV)
    expert_ids = jax.vmap(lambda own, number: assign_block(jax.random.fold_in(own_keys[1], 2), own, number, TOK_DEV, EXPERTS, 2, CAP, 2))(expert_ids_keys, expert_ids_turns).reshape((TOKENS, 2))
    gate_weights = jnp.clip(0.2 + 0.8 * jax.random.uniform(own_keys[2], (TOKENS, 2), jnp.float32) ** levels(own_keys[2], (TOKENS, 2), ((0, 16),), -0.2, 0.2), 0.2, 1.0)
    gate_proj = scatter_about(arg_keys[3], (EXPERTS, D, FF), D ** -0.5, 0.109375, ((0, 4), (2, 4)))
    up_proj = scatter_about(arg_keys[4], (EXPERTS, D, FF), D ** -0.5, 0.109375, ((0, 4), (2, 4)))
    down_proj = scatter_about(arg_keys[5], (EXPERTS, FF, D), FF ** -0.5, 0.0625, ((0, 4), (1, 4)))
    return {"tokens": tokens, "expert_ids": expert_ids, "gate_weights": gate_weights, "gate_proj": gate_proj, "up_proj": up_proj, "down_proj": down_proj}


def expert_rows(rows, w_gate, w_up, w_down):
    gate = jnp.dot(rows, w_gate, preferred_element_type=jnp.float32)
    upward = jnp.dot(rows, w_up, preferred_element_type=jnp.float32)
    hidden = (jax.nn.silu(gate) * upward).astype(jnp.bfloat16)
    group = FF // N_TENSOR
    total = jnp.zeros((rows.shape[0], D), jnp.float32)
    for index in range(N_TENSOR):
        part_hidden = hidden[:, index * group:(index + 1) * group]
        part_down = w_down[index * group:(index + 1) * group]
        partial_value = jnp.dot(part_hidden, part_down, preferred_element_type=jnp.float32).astype(jnp.bfloat16)
        total = total + partial_value.astype(jnp.float32)
    return total.astype(jnp.bfloat16)


def reference(tokens, expert_ids, gate_weights, gate_proj, up_proj, down_proj):
    blocks = TOKENS // TOK_DEV
    ids = expert_ids.reshape(blocks, 2 * TOK_DEV).astype(jnp.int32)
    onehot = (ids[:, :, None] == jnp.arange(EXPERTS, dtype=jnp.int32)[None, None, :]).astype(jnp.int32)
    earlier = jnp.cumsum(onehot, axis=1) - onehot
    slots = jnp.sum(onehot * earlier, axis=2)
    target = ids * CAP + slots
    placed = (target[:, :, None] == jnp.arange(EXPERTS * CAP, dtype=jnp.int32)[None, None, :]).astype(jnp.float32)
    doubled = jnp.repeat(tokens.reshape(blocks, TOK_DEV, D).astype(jnp.float32), 2, axis=1)
    buffer = jnp.einsum("brs,brd->bsd", placed, doubled, precision=lax.Precision.HIGHEST).astype(jnp.bfloat16)
    per_expert = buffer.reshape(blocks, EXPERTS, CAP, D).transpose(1, 0, 2, 3).reshape(EXPERTS, blocks * CAP, D)
    outputs = lax.map(lambda items: expert_rows(items[0], items[1], items[2], items[3]),
                      (per_expert, gate_proj, up_proj, down_proj))
    back = outputs.reshape(EXPERTS, blocks, CAP, D).transpose(1, 0, 2, 3).reshape(blocks, EXPERTS * CAP, D)
    weights = placed * gate_weights.reshape(blocks, 2 * TOK_DEV)[:, :, None]
    contrib = jnp.einsum("brs,bsd->brd", weights, back.astype(jnp.float32), precision=lax.Precision.HIGHEST)
    return contrib.reshape(blocks, TOK_DEV, 2, D).sum(axis=2).reshape(TOKENS, D).astype(jnp.bfloat16)
```

```python
import functools

import jax
import jax.numpy as jnp
from jax import lax
from jax.experimental import pallas as pl
from jax.experimental.pallas import tpu as pltpu
from jax.sharding import PartitionSpec as P

F32 = jnp.float32
BF16 = jnp.bfloat16
LANES = 128
MESH = pl.DeviceIdType.MESH


def chunk_width(total, most):
    width = most
    while total % width:
        width -= LANES
    return width


def layer(n_e, n_y, tok_ref, ids_ref, gw_ref, gate_ref, up_ref, down_ref, out_ref,
          xb, x, wts, hid, wg, wu, wd, part, core_in, mid, y_in, fin, z_in,
          tok_sem, g_sem, u_sem, d_sem,
          agz_s, agz_r, agy_s, agy_r, agc_s, agc_r,
          rc_s, rc_r, ry_s, ry_r, rz_s, rz_r):
    e = lax.axis_index("expert")
    t = lax.axis_index("tensor")
    y = t // 2
    c = t % 2
    rows, width = x.shape
    n_f, _, f_w = wg.shape
    n_d, _, d_w = wd.shape

    def slot(cc, yy, ee):
        return (cc * n_y + yy) * n_e + ee

    me = slot(c, y, e)
    others_e = [(e + k) % n_e for k in range(1, n_e)]
    others_y = [(y + k) % n_y for k in range(1, n_y)]
    partner = {"tensor": y * 2 + 1 - c}

    tok = pltpu.make_async_copy(tok_ref, xb.at[me, :, pl.ds(0, width)], tok_sem)
    tok.start()
    barrier = pltpu.get_barrier_semaphore()
    pl.semaphore_signal(barrier, inc=1, device_id=partner, device_id_type=MESH)
    for yy in others_y:
        pl.semaphore_signal(barrier, inc=1, device_id={"tensor": yy * 2 + c}, device_id_type=MESH)
    for ee in others_e:
        pl.semaphore_signal(barrier, inc=1, device_id={"expert": ee}, device_id_type=MESH)

    lane = lax.broadcasted_iota(jnp.int32, (ids_ref.shape[0], LANES), 1)
    ids = ids_ref[...]
    gw = gw_ref[...]
    w = jnp.where(ids[:, 0:1] == lane, gw[:, 0:1], 0.0) + jnp.where(ids[:, 1:2] == lane, gw[:, 1:2], 0.0)
    head = w.astype(BF16)
    xb[me, :, pl.ds(width, LANES)] = head
    xb[me, :, pl.ds(width + LANES, LANES)] = (w - head.astype(F32)).astype(BF16)
    tok.wait()
    pl.semaphore_wait(barrier, 1 + len(others_y) + len(others_e))

    def gather(index, send, recv, device):
        return pltpu.make_async_remote_copy(
            src_ref=xb.at[index], dst_ref=xb.at[index], send_sem=send, recv_sem=recv,
            device_id=device, device_id_type=MESH)

    sends = []

    def start(copy):
        copy.start()
        sends.append(copy)

    def weights(i):
        return (pltpu.make_async_copy(gate_ref.at[0, :, pl.ds(i * f_w, f_w)], wg.at[i], g_sem.at[i]),
                pltpu.make_async_copy(up_ref.at[0, :, pl.ds(i * f_w, f_w)], wu.at[i], u_sem.at[i]))

    def down(i):
        return pltpu.make_async_copy(down_ref.at[0, :, pl.ds(i * d_w, d_w)], wd.at[i], d_sem.at[i])

    for k, ee in enumerate(others_e):
        start(gather(me, agz_s.at[k], agz_r.at[k], {"expert": ee}))
    for k, yy in enumerate(others_y):
        start(gather(me, agy_s.at[k, 0], agy_r.at[k, 0], {"tensor": yy * 2 + c}))
    start(gather(me, agc_s.at[0, 0], agc_r.at[0, 0], partner))
    for i in range(n_f):
        for copy in weights(i):
            copy.start()
    for i in range(n_d):
        down(i).start()

    for k in range(1, n_e):
        source = slot(c, y, (e + n_e - k) % n_e)
        gather(source, agz_s.at[k - 1], agz_r.at[k - 1], {"expert": e}).wait_recv()
        for m, yy in enumerate(others_y):
            start(gather(source, agy_s.at[m, k], agy_r.at[m, k], {"tensor": yy * 2 + c}))
        start(gather(source, agc_s.at[0, k], agc_r.at[0, k], partner))
    for k in range(n_e):
        for m in range(1, n_y):
            source = slot(c, (y + n_y - m) % n_y, (e + n_e - k) % n_e)
            gather(source, agy_s.at[m - 1, k], agy_r.at[m - 1, k], partner).wait_recv()
            start(gather(source, agc_s.at[m, k], agc_r.at[m, k], partner))
    for k in range(n_e):
        for m in range(n_y):
            source = slot(1 - c, (y + n_y - m) % n_y, (e + n_e - k) % n_e)
            gather(source, agc_s.at[m, k], agc_r.at[m, k], partner).wait_recv()

    expert_lane = lax.broadcasted_iota(jnp.int32, (16, LANES), 1) == e

    def gathered(j, carry):
        pair = xb[pl.ds(2 * j, 2)].astype(F32).reshape(16, width + 2 * LANES)
        at = pl.ds(pl.multiple_of(16 * j, 16), 16)
        x[at, :] = pair[:, :width].astype(BF16)
        both = pair[:, width:width + LANES] + pair[:, width + LANES:]
        own = jnp.sum(jnp.where(expert_lane, both, 0.0), axis=1, keepdims=True)
        wts[at, :] = jnp.broadcast_to(own, (16, LANES))
        return carry

    lax.fori_loop(0, rows // 16, gathered, 0)

    def hidden(i, carry):
        pltpu.make_async_copy(gate_ref.at[0, :, pl.ds(0, f_w)], wg.at[i], g_sem.at[i]).wait()
        gate = jnp.dot(x[...], wg[i], preferred_element_type=F32)
        pltpu.make_async_copy(up_ref.at[0, :, pl.ds(0, f_w)], wu.at[i], u_sem.at[i]).wait()
        up = jnp.dot(x[...], wu[i], preferred_element_type=F32)
        value = gate / (1.0 + jnp.exp(-gate)) * up * wts[:, 0:1]
        hid[:, pl.ds(pl.multiple_of(i * f_w, LANES), f_w)] = value.astype(BF16)
        return carry

    lax.fori_loop(0, n_f, hidden, 0)

    def core_copy(i):
        return pltpu.make_async_remote_copy(
            src_ref=part.at[i, 1 - c], dst_ref=core_in.at[i], send_sem=rc_s.at[i], recv_sem=rc_r.at[i],
            device_id=partner, device_id_type=MESH)

    def y_copy(i, k, yy):
        return pltpu.make_async_remote_copy(
            src_ref=mid.at[i, yy], dst_ref=y_in.at[i, k], send_sem=ry_s.at[i, k], recv_sem=ry_r.at[i, k],
            device_id={"tensor": yy * 2 + c}, device_id_type=MESH)

    def z_copy(i, k, ee):
        return pltpu.make_async_remote_copy(
            src_ref=fin.at[i, ee], dst_ref=z_in.at[i, k], send_sem=rz_s.at[i, k], recv_sem=rz_r.at[i, k],
            device_id={"expert": ee}, device_id_type=MESH)

    def produce(i):
        down(i).wait()
        value = jnp.dot(hid[...], wd[i], preferred_element_type=F32)
        part[i] = value.reshape(
            part.shape[1:]).astype(BF16)
        start(core_copy(i))

    def over_cores(i):
        core_copy(i).wait_recv()
        mid[i] = (part[i, c].astype(F32) + core_in[i].astype(F32)).astype(BF16)
        for k, yy in enumerate(others_y):
            start(y_copy(i, k, yy))

    def over_y(i):
        total = mid[i, y].astype(F32)
        for k, yy in enumerate(others_y):
            y_copy(i, k, yy).wait_recv()
            total = total + y_in[i, k].astype(F32)
        fin[i] = total.astype(BF16)
        for k, ee in enumerate(others_e):
            start(z_copy(i, k, ee))

    def over_e(i):
        total = fin[i, e].astype(F32)
        for k, ee in enumerate(others_e):
            z_copy(i, k, ee).wait_recv()
            total = total + z_in[i, k].astype(F32)
        out_ref[:, pl.ds(i * d_w, d_w)] = total.astype(BF16)

    lags = ((produce, 0), (over_cores, 2), (over_y, 5), (over_e, 9))
    for step in range(n_d + lags[-1][1]):
        for stage, lag in lags:
            if 0 <= step - lag < n_d:
                stage(step - lag)
    for copy in sends:
        copy.wait_send()


def on_device(tokens, expert_ids, gate_weights, gate_proj, up_proj, down_proj):
    n_e = lax.axis_size("expert")
    n_t = lax.axis_size("tensor")
    n_y = n_t // 2
    local, width = tokens.shape
    ff = gate_proj.shape[2]
    rows = n_e * n_t * local
    f_w = chunk_width(ff, 512)
    d_w = chunk_width(width, 512)
    n_f, n_d = ff // f_w, width // d_w
    hbm = pl.BlockSpec(memory_space=pl.ANY)
    vmem = pl.BlockSpec(memory_space=pltpu.VMEM)
    dma = pltpu.SemaphoreType.DMA
    return pl.pallas_call(
        functools.partial(layer, n_e, n_y),
        out_shape=jax.ShapeDtypeStruct((local, width), BF16),
        in_specs=[hbm, vmem, vmem, hbm, hbm, hbm],
        out_specs=vmem,
        scratch_shapes=[
            pltpu.VMEM((n_e * n_t, local, width + 2 * LANES), BF16),
            pltpu.VMEM((rows, width), BF16),
            pltpu.VMEM((rows, LANES), F32),
            pltpu.VMEM((rows, ff), BF16),
            pltpu.VMEM((n_f, width, f_w), BF16),
            pltpu.VMEM((n_f, width, f_w), BF16),
            pltpu.VMEM((n_d, ff, d_w), BF16),
            pltpu.VMEM((n_d, 2, n_y, n_e, local, d_w), BF16),
            pltpu.VMEM((n_d, n_y, n_e, local, d_w), BF16),
            pltpu.VMEM((n_d, n_y, n_e, local, d_w), BF16),
            pltpu.VMEM((n_d, max(1, n_y - 1), n_e, local, d_w), BF16),
            pltpu.VMEM((n_d, n_e, local, d_w), BF16),
            pltpu.VMEM((n_d, max(1, n_e - 1), local, d_w), BF16),
            dma, dma((n_f,)), dma((n_f,)), dma((n_d,)),
            dma((n_e,)), dma((n_e,)),
            dma((n_y, n_e)), dma((n_y, n_e)),
            dma((n_y, n_e)), dma((n_y, n_e)),
            dma((n_d,)), dma((n_d,)),
            dma((n_d, n_y)), dma((n_d, n_y)),
            dma((n_d, n_e)), dma((n_d, n_e)),
        ],
        compiler_params=pltpu.CompilerParams(
            collective_id=0, has_side_effects=True, vmem_limit_bytes=64000 * 1024),
    )(tokens, expert_ids, gate_weights, gate_proj, up_proj, down_proj)


def solution(mesh):
    return jax.shard_map(
        on_device,
        mesh=mesh,
        in_specs=(
            P(("dp", "expert", "tensor"), None),
            P(("dp", "expert", "tensor"), None),
            P(("dp", "expert", "tensor"), None),
            P("expert", None, "tensor"),
            P("expert", None, "tensor"),
            P("expert", "tensor", None),
        ),
        out_specs=P(("dp", "expert", "tensor"), None),
        check_vma=False,
    )
```

```python
import functools

import jax
import jax.numpy as jnp
from jax import lax
from jax.experimental import pallas as pl
from jax.experimental.pallas import tpu as pltpu
from jax.sharding import PartitionSpec as P

F32 = jnp.float32
BF16 = jnp.bfloat16
LANES = 128
DEPTH_MOST = 1536
F_MOST = 2048
MESH = pl.DeviceIdType.MESH


def chunk_width(total, most):
    width = most
    while total % width:
        width -= LANES
    return width


def layer(n_e, n_y, tok_ref, ids_ref, gw_ref, gate_ref, up_ref, down_ref, out_ref,
          xb, x, wts, gates, ups, hid, wg, wu, wd, part, core_in, mid, y_in, fin, z_in,
          tok_sem, g_sem, u_sem, d_sem,
          agz_s, agz_r, agy_s, agy_r, agc_s, agc_r,
          rc_s, rc_r, ry_s, ry_r, rz_s, rz_r):
    e = lax.axis_index("expert")
    t = lax.axis_index("tensor")
    y = t // 2
    c = t % 2
    rows, width = x.shape
    n_p, depth, ff = wg.shape
    f_w = chunk_width(ff, F_MOST)
    n_d, _, d_w = wd.shape

    def slot(cc, yy, ee):
        return (cc * n_y + yy) * n_e + ee

    me = slot(c, y, e)
    upper = e // (n_e // 2)
    mirrored = e + upper * (n_e - 1 - 2 * e)
    others_e = [j + (j + n_e - mirrored) // n_e for j in range(n_e - 1)]
    others_e = [q + upper * (n_e - 1 - 2 * q) for q in others_e]
    others_y = [(y + k) % n_y for k in range(1, n_y)]
    partner = {"tensor": y * 2 + 1 - c}

    tok = pltpu.make_async_copy(tok_ref, xb.at[me, :, pl.ds(0, width)], tok_sem)
    tok.start()
    barrier = pltpu.get_barrier_semaphore()
    pl.semaphore_signal(barrier, inc=1, device_id=partner, device_id_type=MESH)
    for yy in others_y:
        pl.semaphore_signal(barrier, inc=1, device_id={"tensor": yy * 2 + c}, device_id_type=MESH)
    for ee in others_e:
        pl.semaphore_signal(barrier, inc=1, device_id={"expert": ee}, device_id_type=MESH)

    lane = lax.broadcasted_iota(jnp.int32, (ids_ref.shape[1], LANES), 1)
    ids = ids_ref[...].T
    gw = gw_ref[...].T
    w = jnp.where(ids[:, 0:1] == lane, gw[:, 0:1], 0.0) + jnp.where(ids[:, 1:2] == lane, gw[:, 1:2], 0.0)
    head = w.astype(BF16)
    xb[me, :, pl.ds(width, LANES)] = head
    xb[me, :, pl.ds(width + LANES, LANES)] = (w - head.astype(F32)).astype(BF16)
    tok.wait()
    pl.semaphore_wait(barrier, 1 + len(others_y) + len(others_e))

    def gather(p, index, send, recv, device):
        at = xb.at[index, :, pl.ds(p * depth, depth + (2 * LANES if p == n_p - 1 else 0))]
        return pltpu.make_async_remote_copy(
            src_ref=at, dst_ref=at, send_sem=send.at[p], recv_sem=recv.at[p],
            device_id=device, device_id_type=MESH)

    sends = []

    def start(copy):
        copy.start()
        sends.append(copy)

    def gate_copy(p):
        return pltpu.make_async_copy(gate_ref.at[0, pl.ds(p * depth, depth), :], wg.at[p], g_sem.at[p])

    def up_copy(p):
        return pltpu.make_async_copy(up_ref.at[0, pl.ds(p * depth, depth), :], wu.at[p], u_sem.at[p])

    def down(i):
        return pltpu.make_async_copy(down_ref.at[0, :, pl.ds(i * d_w, d_w)], wd.at[i], d_sem.at[i])

    for p in range(n_p):
        for ee in others_e:
            start(gather(p, me, agz_s.at[ee], agz_r.at[e], {"expert": ee}))
        for m, yy in enumerate(others_y):
            start(gather(p, me, agy_s.at[m, e], agy_r.at[m, e], {"tensor": yy * 2 + c}))
        start(gather(p, me, agc_s.at[0, e], agc_r.at[0, e], partner))
    for p in range(n_p):
        gate_copy(p).start()
        up_copy(p).start()
    for i in range(n_d):
        down(i).start()

    def from_e(p):
        for ee in others_e:
            source = slot(c, y, ee)
            gather(p, source, agz_s.at[ee], agz_r.at[ee], partner).wait_recv()
            for m, yy in enumerate(others_y):
                start(gather(p, source, agy_s.at[m, ee], agy_r.at[m, ee], {"tensor": yy * 2 + c}))
            start(gather(p, source, agc_s.at[0, ee], agc_r.at[0, ee], partner))

    def from_y(p):
        for ee in [e] + others_e:
            for m in range(1, n_y):
                source = slot(c, (y + n_y - m) % n_y, ee)
                gather(p, source, agy_s.at[m - 1, ee], agy_r.at[m - 1, ee], partner).wait_recv()
                start(gather(p, source, agc_s.at[m, ee], agc_r.at[m, ee], partner))

    expert_lane = lax.broadcasted_iota(jnp.int32, (16, LANES), 1) == e

    def from_core(p):
        for ee in [e] + others_e:
            for m in range(n_y):
                source = slot(1 - c, (y + n_y - m) % n_y, ee)
                gather(p, source, agc_s.at[m, ee], agc_r.at[m, ee], partner).wait_recv()
        last = p == n_p - 1

        def gathered(j, carry):
            at = pl.ds(pl.multiple_of(16 * j, 16), 16)
            pair = xb[pl.ds(2 * j, 2), :, pl.ds(p * depth, depth)]
            x[at, pl.ds(p * depth, depth)] = pair.astype(F32).reshape(16, depth).astype(BF16)
            if last:
                both = xb[pl.ds(2 * j, 2), :, pl.ds(width, 2 * LANES)].astype(F32).reshape(16, 2 * LANES)
                own = jnp.where(expert_lane, both[:, :LANES] + both[:, LANES:], 0.0)
                wts[at, :] = jnp.broadcast_to(jnp.sum(own, axis=1, keepdims=True), (16, LANES))
            return carry

        lax.fori_loop(0, rows // 16, gathered, 0)
        gate_copy(p).wait()
        up_copy(p).wait()

        def columns(j, carry):
            at = pl.ds(pl.multiple_of(j * f_w, LANES), f_w)
            rows_in = x[:, pl.ds(p * depth, depth)]
            gate = jnp.dot(rows_in, wg[p, :, at], preferred_element_type=F32)
            up = jnp.dot(rows_in, wu[p, :, at], preferred_element_type=F32)
            if p > 0:
                gate = gate + gates[:, at]
                up = up + ups[:, at]
            if last:
                hid[:, at] = (gate / (1.0 + jnp.exp(-gate)) * up * wts[:, 0:1]).astype(BF16)
            else:
                gates[:, at] = gate
                ups[:, at] = up
            return carry

        lax.fori_loop(0, ff // f_w, columns, 0)

    for step in range(n_p + 3):
        for stage, lag in ((from_e, 0), (from_y, 1), (from_core, 2)):
            if 0 <= step - lag < n_p:
                stage(step - lag)

    def core_copy(i):
        return pltpu.make_async_remote_copy(
            src_ref=part.at[i, 1 - c], dst_ref=core_in.at[i], send_sem=rc_s.at[i], recv_sem=rc_r.at[i],
            device_id=partner, device_id_type=MESH)

    def y_copy(i, k, yy):
        return pltpu.make_async_remote_copy(
            src_ref=mid.at[i, yy], dst_ref=y_in.at[i, k], send_sem=ry_s.at[i, k], recv_sem=ry_r.at[i, k],
            device_id={"tensor": yy * 2 + c}, device_id_type=MESH)

    def z_copy(i, to, source):
        return pltpu.make_async_remote_copy(
            src_ref=fin.at[i, to], dst_ref=z_in.at[i, source], send_sem=rz_s.at[i, to],
            recv_sem=rz_r.at[i, source], device_id={"expert": to}, device_id_type=MESH)

    def produce(i):
        down(i).wait()
        value = jnp.dot(hid[...], wd[i], preferred_element_type=F32)
        part[i] = value.reshape(
            part.shape[1:]).astype(BF16)
        start(core_copy(i))

    def over_cores(i):
        core_copy(i).wait_recv()
        mid[i] = (part[i, c].astype(F32) + core_in[i].astype(F32)).astype(BF16)
        for k, yy in enumerate(others_y):
            start(y_copy(i, k, yy))

    def over_y(i):
        total = mid[i, y].astype(F32)
        for k, yy in enumerate(others_y):
            y_copy(i, k, yy).wait_recv()
            total = total + y_in[i, k].astype(F32)
        fin[i] = total.astype(BF16)
        for ee in reversed(others_e):
            start(z_copy(i, ee, e))

    def over_e(i):
        total = fin[i, e].astype(F32)
        for ee in others_e:
            z_copy(i, ee, ee).wait_recv()
            total = total + z_in[i, ee].astype(F32)
        out_ref[:, pl.ds(i * d_w, d_w)] = total.astype(BF16)

    lags = ((produce, 0), (over_cores, 1), (over_y, 5), (over_e, 11))
    for step in range(n_d + lags[-1][1]):
        for stage, lag in lags:
            if 0 <= step - lag < n_d:
                stage(step - lag)
    for copy in sends:
        copy.wait_send()


def on_device(tokens, expert_ids, gate_weights, gate_proj, up_proj, down_proj):
    n_e = lax.axis_size("expert")
    n_t = lax.axis_size("tensor")
    n_y = n_t // 2
    local, width = tokens.shape
    ff = gate_proj.shape[2]
    rows = n_e * n_t * local
    depth = chunk_width(width, DEPTH_MOST)
    d_w = chunk_width(width, 512)
    n_p, n_d = width // depth, width // d_w
    hbm = pl.BlockSpec(memory_space=pl.ANY)
    vmem = pl.BlockSpec(memory_space=pltpu.VMEM)
    dma = pltpu.SemaphoreType.DMA
    return pl.pallas_call(
        functools.partial(layer, n_e, n_y),
        out_shape=jax.ShapeDtypeStruct((local, width), BF16),
        in_specs=[hbm, vmem, vmem, hbm, hbm, hbm],
        out_specs=vmem,
        scratch_shapes=[
            pltpu.VMEM((n_e * n_t, local, width + 2 * LANES), BF16),
            pltpu.VMEM((rows, width), BF16),
            pltpu.VMEM((rows, LANES), F32),
            pltpu.VMEM((rows, ff), F32),
            pltpu.VMEM((rows, ff), F32),
            pltpu.VMEM((rows, ff), BF16),
            pltpu.VMEM((n_p, depth, ff), BF16),
            pltpu.VMEM((n_p, depth, ff), BF16),
            pltpu.VMEM((n_d, ff, d_w), BF16),
            pltpu.VMEM((n_d, 2, n_y, n_e, local, d_w), BF16),
            pltpu.VMEM((n_d, n_y, n_e, local, d_w), BF16),
            pltpu.VMEM((n_d, n_y, n_e, local, d_w), BF16),
            pltpu.VMEM((n_d, max(1, n_y - 1), n_e, local, d_w), BF16),
            pltpu.VMEM((n_d, n_e, local, d_w), BF16),
            pltpu.VMEM((n_d, n_e, local, d_w), BF16),
            dma, dma((n_p,)), dma((n_p,)), dma((n_d,)),
            dma((n_e, n_p)), dma((n_e, n_p)),
            dma((n_y, n_e, n_p)), dma((n_y, n_e, n_p)),
            dma((n_y, n_e, n_p)), dma((n_y, n_e, n_p)),
            dma((n_d,)), dma((n_d,)),
            dma((n_d, n_y)), dma((n_d, n_y)),
            dma((n_d, n_e)), dma((n_d, n_e)),
        ],
        compiler_params=pltpu.CompilerParams(
            collective_id=0, has_side_effects=True, vmem_limit_bytes=64000 * 1024),
    )(tokens, expert_ids.T, gate_weights.T, gate_proj, up_proj, down_proj)


def solution(mesh):
    return jax.shard_map(
        on_device,
        mesh=mesh,
        in_specs=(
            P(("dp", "expert", "tensor"), None),
            P(("dp", "expert", "tensor"), None),
            P(("dp", "expert", "tensor"), None),
            P("expert", None, "tensor"),
            P("expert", None, "tensor"),
            P("expert", "tensor", None),
        ),
        out_specs=P(("dp", "expert", "tensor"), None),
        check_vma=False,
    )
```
